1024 devices in a mesh: shard: 128 (over z, x, y_lo), rep: 8 (over y_hi, core).
Axes of the slice: x: 4, y: 8 (y_hi: 4, y_lo: 2; y = y_hi * 2 + y_lo), z: 16, core: 2. Of those that a mesh axis runs over, the one named last changes fastest.
Arguments:
- activations: bfloat16 [4, 65536, 2048], P(None, ('shard', 'rep')), may hold values from -24 to 24
- value_grad: bfloat16 [4, 65536, 512], P(None, ('shard', 'rep')), may hold values from -6 to 6
- norm_gain: bfloat16 [2048], P('shard'), may hold values from 0.25 to 4.5
- value_weight: bfloat16 [2048, 512], P('shard'), may hold values from -0.125 to 0.125
Outputs:
- input_grad: bfloat16 [4, 65536, 2048], P(None, ('shard', 'rep'))
- weight_update: float32 [2048, 512], P('shard')
The draws below stay inside these ranges and needn't reach their ends.
All inputs are finite; a program needn't handle non-finite values.
Results may differ from the reference program's by a relative error of at most 0.0029.
Values may be sent and summed in bfloat16 or wider, within the bound.
A program may use at most 32 MiB of HBM per device.

```python
import jax
import jax.numpy as jnp
from jax import lax

D = 2048
VW = 512
MB = 4
TOKENS = 65536


def draw_norm_gain(key, part):
    where = jnp.arange(D, dtype=jnp.float32) / D
    noise = jax.random.uniform(key, (D,), jnp.float32, -0.4, 0.4)
    base = 0.6 + 1.2 * where
    return (base * jnp.exp(noise)).astype(jnp.bfloat16)


def spiked(values, key, source, target, shards_of, factor):
    owner, partner = [(jnp.arange(values.shape[position]) // (values.shape[position] // shards_of)).reshape([-1 if axis == position else 1 for axis in range(values.ndim)]) for position in (source, target)]
    chosen = jax.random.permutation(key, shards_of)[partner]
    strong = (owner == chosen) | (owner == (partner + shards_of // 2) % shards_of)
    return jnp.where(strong, factor * values, values)


def level_of(stream_key, extent, cuts, low, largest):
    def one(axis_at, parts):
        steps = jax.random.uniform(jax.random.fold_in(jax.random.fold_in(stream_key, 6), axis_at), (parts,), jnp.float32, low / len(cuts), largest / len(cuts))
        return jnp.repeat(jnp.exp(steps), extent[axis_at] // parts).reshape((-1,) + (1,) * (len(extent) - axis_at - 1))

    factor_of = one(*cuts[0])
    for cut in cuts[1:]:
        factor_of = factor_of * one(*cut)
    return factor_of


def bell_draw(own_key, shape, spread, bound, shards=(), kind=jnp.bfloat16):
    loudness = level_of(own_key, shape, shards, -0.22, 0.18) if shards else 1.0
    drawn = jax.random.normal(own_key, shape, jnp.float32) * spread * loudness
    return jnp.minimum(jnp.maximum(drawn, -bound), bound).astype(kind)


def bell_draw_with(key, dims, width, limit, pieces, heavy, kind=jnp.bfloat16):
    entries = width * jax.random.normal(key, dims, jnp.float32)
    if pieces:
        entries = entries * level_of(key, dims, pieces, -0.22, 0.18)
    return jnp.clip(spiked(entries, jax.random.fold_in(key, 3), *heavy), -limit, limit).astype(kind)


def setup_inputs(seed: int = 0) -> dict:
    splits = jax.random.split(jax.random.key(seed), 5)
    return {
        "activations": bell_draw_with(splits[0], (MB, TOKENS, D), 1.0, 24.0, ((1, 1024),), (1, 2, 1024, 6.0)),
        "value_grad": bell_draw(splits[1], (MB, TOKENS, VW), 1.0, 6.0, ((1, 1024),)),
        "norm_gain": draw_norm_gain(jax.random.fold_in(splits[4], 71), 0),
        "value_weight": bell_draw(splits[3], (D, VW), D ** -0.5, 0.125, ((0, 128),)),
    }


def reference(activations, value_grad, norm_gain, value_weight):
    gain = norm_gain.astype(jnp.float32)

    def one_batch(total, inputs):
        block, cotangent = inputs
        values = block.astype(jnp.float32)
        rstd = lax.rsqrt(lax.optimization_barrier(jnp.mean(values * values, axis=-1, keepdims=True)) + 1e-05)
        normed = (values * rstd * gain).astype(jnp.bfloat16)
        total = total + lax.dot_general(normed, cotangent, (((0,), (0,)), ((), ())), preferred_element_type=jnp.float32)
        normed_grad = jnp.dot(cotangent, value_weight.T, preferred_element_type=jnp.float32)
        scaled = normed_grad * gain
        inner = lax.optimization_barrier(jnp.mean(scaled * values, axis=-1, keepdims=True))
        result = (rstd * scaled - values * rstd * rstd * rstd * inner).astype(jnp.bfloat16)
        return (total, result)
    start = jnp.zeros((D, VW), jnp.float32)
    grad, input_grad = lax.scan(one_batch, start, (activations, value_grad))
    squares = jnp.sum(grad * grad)
    factor = 1.0 / jnp.maximum(1.0, jnp.sqrt(squares / (D * VW)))
    return (input_grad, grad * factor)
```

```python
import functools

import jax
import jax.numpy as jnp
from jax import lax
from jax.experimental import pallas as pl
from jax.experimental.pallas import tpu as pltpu
from jax.sharding import Mesh
from jax.sharding import PartitionSpec as P

AXES = ("z", "x", "yl", "yh", "c")
NZ, NX, NYL, NYH, NC = 16, 4, 2, 4, 2
NY = NYL * NYH
MESH = pl.DeviceIdType.MESH
F32, BF16 = jnp.float32, jnp.bfloat16


def kernel(
    x_ref, vg_ref, w_ref, grow_ref, gcol_ref,
    out_ref, upd_ref,
    rstd, hi, lo, g, r, xs, xr, s, yr, s2, zr, gb, sq, sqz, sq2, sqx, wbuf, gbuf, hbuf, gainrow,
    wz_s, wz_r, gz_s, gz_r, wy_s, wy_r, gy_s, gy_r, wx_s, wx_r, gx_s, gx_r, wc_s, wc_r,
    dc_s, dc_r, rx_s, rx_r, ry_s, ry_r, rz_s, rz_r, rg_s, rg_r, qz_s, qz_r, qx_s, qx_r,
):
    iz, ix, il, ih, ic = (lax.axis_index(a) for a in AXES)
    iy = ih * NYL + il
    tokens, width = x_ref.shape
    oc = 1 - ic
    sends = []

    def at_x(k):
        return lax.rem(ix + k, NX)

    def at_y(k):
        return lax.rem(iy + k, NY)

    def at_z(k):
        return lax.rem(iz + k, NZ)

    def to_x(k):
        return {"x": at_x(k)}

    def to_y(k):
        y = at_y(k)
        return {"yh": y // NYL, "yl": lax.rem(y, NYL)}

    def to_z(k):
        return {"z": at_z(k)}

    def to_rep(k):
        return {"yh": lax.rem(ih + k // NC, NYH), "c": lax.rem(ic + k % NC, NC)}

    def to_plane(k):
        return {"x": at_x(k // NYL), "yl": lax.rem(il + k % NYL, NYL)}

    def send(src, dst, ss, rs, dev):
        copy = pltpu.make_async_remote_copy(
            src_ref=src, dst_ref=dst, send_sem=ss, recv_sem=rs, device_id=dev, device_id_type=MESH
        )
        copy.start()
        sends.append(copy)

    def arrived(dst, ss, rs):
        pltpu.make_async_remote_copy(
            src_ref=dst, dst_ref=dst, send_sem=ss, recv_sem=rs, device_id={"c": oc}, device_id_type=MESH
        ).wait_recv()

    barrier = pltpu.get_barrier_semaphore()
    peers = [to_z(k) for k in range(1, NZ)]
    peers += [to_y(k) for k in range(1, NY)]
    peers += [to_x(k) for k in range(1, NX)]
    peers += [to_plane(k) for k in range(1, NX * NYL) if k % NYL and k // NYL]
    peers += [to_rep(k) for k in range(1, NC * NYH) if k % NC]
    for dev in peers:
        pl.semaphore_signal(barrier, inc=1, device_id=dev, device_id_type=MESH)

    block = 32

    @pl.loop(0, tokens // block)
    def _(t):
        rows = pl.ds(pl.multiple_of(t * block, block), block)
        acc = jnp.zeros((block, 128), F32)
        for j in range(width // 128):
            v = x_ref[rows, j * 128 : (j + 1) * 128].astype(F32)
            acc = acc + v * v
        inv = lax.rsqrt(jnp.sum(acc, axis=1, keepdims=True) / width + 1e-05)
        rstd[rows, :] = jnp.broadcast_to(inv, (block, 128))
        scaled = vg_ref[rows, :].astype(F32) * inv
        high = scaled.astype(BF16)
        hi[rows, :] = high
        lo[rows, :] = (scaled - high.astype(F32)).astype(BF16)

    wbuf[ic, iz, ix, il] = w_ref[ic]
    gbuf[iz, ix, il] = grow_ref[...]
    pl.semaphore_wait(barrier, len(peers))

    for k in sorted(range(1, NZ), key=lambda k: -min(k, NZ - k)):
        send(w_ref.at[ic], wbuf.at[ic, iz, ix, il], wz_s.at[k - 1], wz_r.at[k - 1], to_z(k))
        send(grow_ref, gbuf.at[iz, ix, il], gz_s.at[k - 1], gz_r.at[k - 1], to_z(k))

    zs = 2
    feats = zs * 128

    @pl.loop(0, NZ // zs)
    def _(n):
        cols = pl.ds(pl.multiple_of(n * feats, feats), feats)
        xa = x_ref[:, cols]
        for half in range(2):
            hc = slice(half * 256, half * 256 + 256)
            dims = (((0,), (0,)), ((), ()))
            o = lax.dot_general(xa, hi[:, hc], dims, preferred_element_type=F32)
            o = o + lax.dot_general(xa, lo[:, hc], dims, preferred_element_type=F32)
            for zl in range(zs):
                for xx in range(NX):
                    for yl in range(NYL):
                        for cc in range(NC):
                            row = zl * 128 + xx * 32 + yl * 16 + cc * 8
                            for hh in range(2):
                                yy = (half * 2 + hh) * NYL + yl
                                at = pl.ds(pl.multiple_of(n * zs * 8 + zl * 8, 8), 8)
                                g[cc, xx, yy, at, :] = o[row : row + 8, hh * 128 : hh * 128 + 128]
        at = pl.ds(pl.multiple_of(n * zs * 8, 8), zs * 8)
        pltpu.make_async_remote_copy(
            src_ref=g.at[oc, :, :, at],
            dst_ref=r.at[:, :, at],
            send_sem=dc_s.at[n],
            recv_sem=dc_r.at[n],
            device_id={"c": oc},
            device_id_type=MESH,
        ).start()

    @pl.loop(0, NZ // zs)
    def _(n):
        at = pl.ds(pl.multiple_of(n * zs * 8, 8), zs * 8)
        pltpu.make_async_remote_copy(
            src_ref=g.at[oc, :, :, at],
            dst_ref=r.at[:, :, at],
            send_sem=dc_s.at[n],
            recv_sem=dc_r.at[n],
            device_id={"c": oc},
            device_id_type=MESH,
        ).wait()

    for k in (2, 1, 3):
        tx = at_x(k)

        @pl.loop(0, NY)
        def _(y):
            xs[k - 1, y] = (g[ic, tx, y] + r[tx, y]).astype(BF16)

        send(xs.at[k - 1], xr.at[k - 1], rx_s.at[k - 1], rx_r.at[k - 1], to_x(k))

    for k in range(1, NZ):
        fz = at_z(NZ - k)
        arrived(wbuf.at[ic, fz, ix, il], wz_s.at[k - 1], wz_r.at[k - 1])
        arrived(gbuf.at[fz, ix, il], gz_s.at[k - 1], gz_r.at[k - 1])
    send(wbuf.at[ic, :, ix, il], wbuf.at[ic, :, ix, il], wy_s, wy_r, {"yl": 1 - il})
    send(gbuf.at[:, ix, il], gbuf.at[:, ix, il], gy_s, gy_r, {"yl": 1 - il})

    for k in range(1, NX):
        arrived(xr.at[k - 1], rx_s.at[k - 1], rx_r.at[k - 1])

    def x_sum(y):
        total = g[ic, ix, y] + r[ix, y]
        for k in range(1, NX):
            total = total + xr[k - 1, y].astype(F32)
        return total

    for k in (4, 3, 5, 2, 6, 1, 7):
        y = at_y(k)
        s[y] = x_sum(y)
        send(s.at[y], yr.at[k - 1], ry_s.at[k - 1], ry_r.at[k - 1], to_y(k))
    s[iy] = x_sum(iy)

    arrived(wbuf.at[ic, :, ix, 1 - il], wy_s, wy_r)
    arrived(gbuf.at[:, ix, 1 - il], gy_s, gy_r)
    for k in (2, 1, 3):
        send(wbuf.at[ic, :, ix], wbuf.at[ic, :, ix], wx_s.at[k - 1], wx_r.at[k - 1], to_x(k))
        send(gbuf.at[:, ix], gbuf.at[:, ix], gx_s.at[k - 1], gx_r.at[k - 1], to_x(k))
    send(wbuf.at[ic, :, ix], wbuf.at[ic, :, ix], wc_s.at[0], wc_r.at[0], {"c": oc})

    total = s[iy]
    for k in range(1, NY):
        arrived(yr.at[k - 1], ry_s.at[k - 1], ry_r.at[k - 1])
        total = total + yr[k - 1]
    s2[...] = total

    for k in sorted(range(1, NZ), key=lambda k: -min(k, NZ - k)):
        at = pl.ds(pl.multiple_of(at_z(k) * 8, 8), 8)
        send(s2.at[at], zr.at[k - 1], rz_s.at[k - 1], rz_r.at[k - 1], to_z(k))

    for k in (1, 3, 2):
        fx = at_x(NX - k)
        arrived(wbuf.at[ic, :, fx], wx_s.at[k - 1], wx_r.at[k - 1])
        arrived(gbuf.at[:, fx], gx_s.at[k - 1], gx_r.at[k - 1])
        send(wbuf.at[ic, :, fx], wbuf.at[ic, :, fx], wc_s.at[k], wc_r.at[k], {"c": oc})
    for k in range(NX):
        fx = at_x(NX - k)
        arrived(wbuf.at[oc, :, fx], wc_s.at[k], wc_r.at[k])

    for z in range(NZ):
        row = jnp.zeros((1, 128), F32)
        for xx in range(NX):
            for yl in range(NYL):
                row = row + gbuf[z, xx, yl]
        gainrow[:, z * 128 : (z + 1) * 128] = jnp.broadcast_to(row, (8, 128))

    hbuf[:, width:] = jnp.zeros((tokens, 128), F32)

    @pl.loop(0, NZ)
    def _(z):
        cols = pl.ds(pl.multiple_of(z * 128, 128), 128)
        dims = (((1,), (1,)), ((), ()))
        h = jnp.zeros((tokens, 128), F32)
        for half in range(2):
            wt = wbuf[half, z].reshape(128, 256)
            h = h + lax.dot_general(
                vg_ref[:, half * 256 : half * 256 + 256], wt, dims, preferred_element_type=F32
            )
        h = h * gainrow[0:1, cols]
        hbuf[:, cols] = h
        hbuf[:, width:] += h * x_ref[:, cols].astype(F32)

    own = s2[pl.ds(pl.multiple_of(iz * 8, 8), 8), :]
    for k in range(1, NZ):
        arrived(zr.at[k - 1], rz_s.at[k - 1], rz_r.at[k - 1])
        own = own + zr[k - 1]
    gb[ih, ic] = own * gcol_ref[ic]
    for k in range(1, NYH * NC):
        send(gb.at[ih, ic], gb.at[ih, ic], rg_s.at[k - 1], rg_r.at[k - 1], to_rep(k))

    @pl.loop(0, tokens // block)
    def _(t):
        rows = pl.ds(pl.multiple_of(t * block, block), block)
        inner = jnp.sum(hbuf[rows, width:], axis=1, keepdims=True) / width
        inv = rstd[rows, 0:1]
        coef = inv * inv * inv * inner
        for j in range(width // 128):
            cs = slice(j * 128, (j + 1) * 128)
            v = x_ref[rows, cs].astype(F32)
            out_ref[rows, cs] = (inv * hbuf[rows, cs] - v * coef).astype(BF16)

    for k in range(1, NYH * NC):
        fh, fc = lax.rem(ih + NYH - k // NC, NYH), lax.rem(ic + k % NC, NC)
        arrived(gb.at[fh, fc], rg_s.at[k - 1], rg_r.at[k - 1])

    acc = jnp.zeros((8, 128), F32)
    for hh in range(NYH):
        for cc in range(NC):
            acc = acc + gb[hh, cc] * gb[hh, cc]
    sq[...] = acc
    for k in sorted(range(1, NZ), key=lambda k: -min(k, NZ - k)):
        send(sq, sqz.at[k - 1], qz_s.at[k - 1], qz_r.at[k - 1], to_z(k))
    for k in range(1, NZ):
        arrived(sqz.at[k - 1], qz_s.at[k - 1], qz_r.at[k - 1])
        acc = acc + sqz[k - 1]
    sq2[...] = acc
    for k in (5, 4, 3, 7, 2, 6, 1):
        send(sq2, sqx.at[k - 1], qx_s.at[k - 1], qx_r.at[k - 1], to_plane(k))
    for k in range(1, NX * NYL):
        arrived(sqx.at[k - 1], qx_s.at[k - 1], qx_r.at[k - 1])
        acc = acc + sqx[k - 1]
    squares = jnp.sum(jnp.sum(acc, axis=1, keepdims=True), axis=0, keepdims=True)
    factor = 1.0 / jnp.maximum(1.0, jnp.sqrt(squares / (width * 512)))
    for hh in range(NYH):
        for cc in range(NC):
            upd_ref[cc * 8 : cc * 8 + 8, hh * 128 : hh * 128 + 128] = gb[hh, cc] * factor

    for copy in sends:
        copy.wait_send()


def on_device(activations, value_grad, norm_gain, value_weight):
    batch, tok, width = activations.shape
    columns = value_grad.shape[2]
    tokens = batch * tok
    own = norm_gain.shape[0]
    gain = norm_gain.astype(F32)
    place = lax.axis_index("x") * NYL + lax.axis_index("yl")
    lanes = jnp.arange(128) // own == place
    grow = jnp.where(lanes, jnp.tile(gain, 128 // own), 0.0).reshape(1, 128)
    gcol = jnp.broadcast_to(gain.reshape(NC, own // NC, 1), (NC, own // NC, 128))
    weight = jnp.moveaxis(value_weight.reshape(own, NC, columns // NC), 1, 0)
    vm = pl.BlockSpec(memory_space=pltpu.VMEM)

    def dma(n):
        return pltpu.SemaphoreType.DMA((n,))

    def sem(n):
        return [dma(n), dma(n)]

    one = [pltpu.SemaphoreType.DMA, pltpu.SemaphoreType.DMA]
    v = pltpu.VMEM
    scratch = [
        v((tokens, 128), F32),
        v((tokens, columns), BF16),
        v((tokens, columns), BF16),
        v((NC, NX, NY, 128, 128), F32),
        v((NX, NY, 128, 128), F32),
        v((NX - 1, NY, 128, 128), BF16),
        v((NX - 1, NY, 128, 128), BF16),
        v((NY, 128, 128), F32),
        v((NY - 1, 128, 128), F32),
        v((128, 128), F32),
        v((NZ - 1, 8, 128), F32),
        v((NYH, NC, 8, 128), F32),
        v((8, 128), F32),
        v((NZ - 1, 8, 128), F32),
        v((8, 128), F32),
        v((NX * NYL - 1, 8, 128), F32),
        v((NC, NZ, NX, NYL, own, columns // NC), BF16),
        v((NZ, NX, NYL, 1, 128), F32),
        v((tokens, width + 128), F32),
        v((8, width), F32),
        *sem(NZ - 1), *sem(NZ - 1), *one, *one, *sem(NX - 1), *sem(NX - 1), *sem(NX),
        *sem(NZ // 2), *sem(NX - 1), *sem(NY - 1), *sem(NZ - 1), *sem(NYH * NC - 1), *sem(NZ - 1),
        *sem(NX * NYL - 1),
    ]
    result, update = pl.pallas_call(
        kernel,
        out_shape=(
            jax.ShapeDtypeStruct((tokens, width), BF16),
            jax.ShapeDtypeStruct((own, columns), F32),
        ),
        in_specs=[vm] * 5,
        out_specs=(vm, vm),
        scratch_shapes=scratch,
        compiler_params=pltpu.CompilerParams(
            collective_id=0, has_side_effects=True, vmem_limit_bytes=48 * 1024 * 1024
        ),
        name="normed_value_backward",
    )(activations.reshape(tokens, width), value_grad.reshape(tokens, columns), weight, grow, gcol)
    return result.reshape(activations.shape), update


def solution(mesh):
    split = Mesh(mesh.devices.reshape(NZ, NX, NYL, NYH, NC), AXES)
    rows = ("z", "x", "yl")
    placed = (P(None, AXES, None), P(None, AXES, None), P(rows), P(rows, None))
    return jax.shard_map(
        on_device,
        mesh=split,
        in_specs=placed,
        out_specs=(P(None, AXES, None), P(rows, None)),
        check_vma=False,
    )
```

```python
import jax
import jax.numpy as jnp
from jax import lax
from jax.experimental import pallas as pl
from jax.experimental.pallas import tpu as pltpu
from jax.sharding import Mesh
from jax.sharding import PartitionSpec as P

AXES = ("z", "x", "yl", "yh", "c")
NZ, NX, NYL, NYH, NC = 16, 4, 2, 4, 2
NY = NYL * NYH
NG = NZ // 2
FAR = (4, 3, 5)
NEAR = (2, 6, 1, 7)
MESH = pl.DeviceIdType.MESH
F32, BF16 = jnp.float32, jnp.bfloat16


def kernel(
    x_hbm, vg_hbm, w_ref, grow_ref, gcol_ref,
    out_ref, upd_ref,
    x_ref, vg_ref, rstd, hi, lo, g, r, xs, xr, s, sb, yr, yb, s2, zr, gb, sqp, sqz,
    wbuf, gbuf, hbuf, gainrow,
    ld, wz_s, wz_r, gz_s, gz_r, wy_s, wy_r, gy_s, gy_r, wx_s, wx_r, gx_s, gx_r, wc_s, wc_r,
    dc_s, dc_r, rx_s, rx_r, ry_s, ry_r, rz_s, rz_r, rg_s, rg_r, qp_s, qp_r, qz_s, qz_r,
):
    iz, ix, il, ih, ic = (lax.axis_index(a) for a in AXES)
    iy = ih * NYL + il
    parity = lax.rem(iz, 2)
    tokens, width = x_ref.shape
    oc = 1 - ic
    sibling = {"c": oc}
    sends = []

    def at_x(k):
        return lax.rem(ix + k, NX)

    def at_y(k):
        return lax.rem(iy + k, NY)

    def at_z(k):
        return lax.rem(iz + k, NZ)

    def to_x(k):
        return {"x": at_x(k)}

    def to_y(k):
        y = at_y(k)
        return {"yh": y // NYL, "yl": lax.rem(y, NYL)}

    def to_rep(k):
        return {"yh": lax.rem(ih + k // NC, NYH), "c": lax.rem(ic + k % NC, NC)}

    def to_plane(k):
        return {"x": at_x(k // NY), **to_y(k % NY)}

    def to_column(k):
        return {"z": at_z(k // NC), "c": lax.rem(ic + k % NC, NC)}

    def remote(src, dst, ss, rs, dev):
        return pltpu.make_async_remote_copy(
            src_ref=src, dst_ref=dst, send_sem=ss, recv_sem=rs, device_id=dev, device_id_type=MESH
        )

    def send(*args):
        copy = remote(*args)
        copy.start()
        sends.append(copy)

    def arrived(dst, ss, rs):
        remote(dst, dst, ss, rs, sibling).wait_recv()

    barrier = pltpu.get_barrier_semaphore()
    peers = [to_column(k) for k in range(1, NZ * NC)]
    peers += [to_plane(k) for k in range(1, NX * NY)]
    peers += [to_rep(k) for k in range(1, NYH * NC) if k % NC and k // NC]
    for dev in peers:
        pl.semaphore_signal(barrier, inc=1, device_id=dev, device_id_type=MESH)

    parts = ld.shape[0] - 1
    chunk = tokens // parts
    loads = [
        pltpu.make_async_copy(
            x_hbm.at[pl.ds(t * chunk, chunk)], x_ref.at[pl.ds(t * chunk, chunk)], ld.at[t]
        )
        for t in range(parts)
    ]
    loads.append(pltpu.make_async_copy(vg_hbm, vg_ref, ld.at[parts]))
    for t in (0, parts, *range(1, parts)):
        loads[t].start()
    wbuf[ic, iz, ix, il] = w_ref[ic]
    gbuf[iz, ix, il] = grow_ref[...]

    block = 32
    for t in range(parts):
        loads[t].wait()
        if t == 0:
            loads[parts].wait()

        @pl.loop(t * chunk // block, (t + 1) * chunk // block)
        def _(b):
            rows = pl.ds(pl.multiple_of(b * block, block), block)
            acc = jnp.zeros((block, 128), F32)
            for j in range(width // 128):
                v = x_ref[rows, j * 128 : (j + 1) * 128].astype(F32)
                acc = acc + v * v
            inv = lax.rsqrt(jnp.sum(acc, axis=1, keepdims=True) / width + 1e-05)
            rstd[rows, :] = jnp.broadcast_to(inv, (block, 128))
            scaled = vg_ref[rows, :].astype(F32) * inv
            high = scaled.astype(BF16)
            hi[rows, :] = high
            lo[rows, :] = (scaled - high.astype(F32)).astype(BF16)

    def group(n):
        half = (n + 1) // 2
        return lax.rem(iz // 2 + NG // 2 + half * (1 - 2 * (n % 2)), NG)

    def gradient(n):
        cols = pl.ds(pl.multiple_of(group(n) * 256, 256), 256)
        xa = x_ref[:, cols]
        for half in range(2):
            hc = slice(half * 256, half * 256 + 256)
            dims = (((0,), (0,)), ((), ()))
            o = lax.dot_general(xa, hi[:, hc], dims, preferred_element_type=F32)
            o = o + lax.dot_general(xa, lo[:, hc], dims, preferred_element_type=F32)
            for zl in range(2):
                for xx in range(NX):
                    for yl in range(NYL):
                        for cc in range(NC):
                            row = zl * 128 + xx * 32 + yl * 16 + cc * 8
                            for hh in range(2):
                                yy = (half * 2 + hh) * NYL + yl
                                g[cc, n, xx, yy, zl * 8 : zl * 8 + 8, :] = o[
                                    row : row + 8, hh * 128 : hh * 128 + 128
                                ]

    def core_copy(n):
        return remote(g.at[oc, n], r.at[n], dc_s.at[n], dc_r.at[n], sibling)

    def x_copy(k, n):
        return remote(
            xs.at[k - 1, n], xr.at[k - 1, n], rx_s.at[k - 1, n], rx_r.at[k - 1, n], to_x(k)
        )

    def y_copy(k, n):
        y = at_y(k)
        if k in FAR:
            j = FAR.index(k)
            src, dst = sb.at[j, n], yb.at[j, n]
        else:
            src, dst = s.at[n, y], yr.at[NEAR.index(k), n]
        return remote(src, dst, ry_s.at[k - 1, n], ry_r.at[k - 1, n], to_y(k))

    def z_copy(zl, n):
        rows = pl.ds(pl.multiple_of(zl * 8, 8), 8)
        return remote(
            s2.at[n, rows], zr.at[iz], rz_s.at[n, zl], rz_r.at[iz], {"z": group(n) * 2 + zl}
        )

    def reduce_x(n):
        core_copy(n).wait_recv()
        for k in (2, 1, 3):
            tx = at_x(k)
            xs[k - 1, n] = (g[ic, n, tx] + r[n, tx]).astype(BF16)
            x_copy(k, n).start()

    def reduce_y(n):
        for k in range(1, NX):
            x_copy(k, n).wait_recv()
        total = g[ic, n, ix] + r[n, ix]
        for k in range(1, NX):
            total = total + xr[k - 1, n].astype(F32)
        s[n] = total
        for j, k in enumerate(FAR):
            sb[j, n] = s[n, at_y(k)].astype(BF16)
        for k in FAR + NEAR:
            y_copy(k, n).start()

    def reduce_z(n):
        total = s[n, iy]
        for k in FAR + NEAR:
            y_copy(k, n).wait_recv()
            total = total + (
                yb[FAR.index(k), n].astype(F32) if k in FAR else yr[NEAR.index(k), n]
            )
        s2[n] = total

    gradient(0)
    gradient(1)
    pl.semaphore_wait(barrier, len(peers))
    core_copy(0).start()
    core_copy(1).start()

    for k in sorted(range(1, NZ), key=lambda k: -min(k, NZ - k)):
        dev = {"z": at_z(k)}
        send(w_ref.at[ic], wbuf.at[ic, iz, ix, il], wz_s.at[k - 1], wz_r.at[k - 1], dev)
        send(grow_ref, gbuf.at[iz, ix, il], gz_s.at[k - 1], gz_r.at[k - 1], dev)

    lag = 3

    @pl.loop(2, NG)
    def _(n):
        gradient(n)
        core_copy(n).start()

        @pl.when(n >= lag)
        def _():
            reduce_x(n - lag)

    @pl.loop(NG - lag, NG)
    def _(n):
        reduce_x(n)

    @pl.loop(0, 3)
    def _(n):
        reduce_y(n)

    for k in range(1, NZ):
        fz = at_z(NZ - k)
        arrived(wbuf.at[ic, fz, ix, il], wz_s.at[k - 1], wz_r.at[k - 1])
        arrived(gbuf.at[fz, ix, il], gz_s.at[k - 1], gz_r.at[k - 1])
    send(wbuf.at[ic, :, ix, il], wbuf.at[ic, :, ix, il], wy_s, wy_r, {"yl": 1 - il})
    send(gbuf.at[:, ix, il], gbuf.at[:, ix, il], gy_s, gy_r, {"yl": 1 - il})

    behind = 3

    @pl.loop(3, NG)
    def _(n):
        reduce_y(n)
        reduce_z(n - behind)
        for zl in range(2):
            z_copy(zl, n - behind).start()

    arrived(wbuf.at[ic, :, ix, 1 - il], wy_s, wy_r)
    arrived(gbuf.at[:, ix, 1 - il], gy_s, gy_r)
    for k in (2, 1, 3):
        send(wbuf.at[ic, :, ix], wbuf.at[ic, :, ix], wx_s.at[k - 1], wx_r.at[k - 1], to_x(k))
        send(gbuf.at[:, ix], gbuf.at[:, ix], gx_s.at[k - 1], gx_r.at[k - 1], to_x(k))
    send(wbuf.at[ic, :, ix], wbuf.at[ic, :, ix], wc_s.at[0], wc_r.at[0], sibling)

    @pl.loop(NG - behind, NG - 1)
    def _(n):
        reduce_z(n)
        for zl in range(2):
            z_copy(zl, n).start()

    reduce_z(NG - 1)
    z_copy(1 - parity, NG - 1).start()

    own = s2[NG - 1, pl.ds(pl.multiple_of(parity * 8, 8), 8), :]
    for k in sorted(range(1, NZ), key=lambda k: -min(k, NZ - k)):
        fz = at_z(k)
        arrived(zr.at[fz], rz_s.at[0, 0], rz_r.at[fz])
        own = own + zr[fz]
    piece = own * gcol_ref[ic]
    gb[ih, ic] = piece
    here = ix * NY + iy
    sqp[here] = jnp.sum(piece * piece, axis=0, keepdims=True)
    for k in sorted(range(1, NX * NY), key=lambda k: -min(k % NY, NY - k % NY)):
        send(sqp.at[here], sqp.at[here], qp_s.at[k - 1], qp_r.at[here], to_plane(k))
    for k in range(1, NYH * NC):
        send(gb.at[ih, ic], gb.at[ih, ic], rg_s.at[k - 1], rg_r.at[k - 1], to_rep(k))
    for k in range(1, NX * NY):
        there = at_x(k // NY) * NY + at_y(k % NY)
        arrived(sqp.at[there], qp_s.at[0], qp_r.at[there])
    row = sqp[0]
    for k in range(1, NX * NY):
        row = row + sqp[k]

    there = iz * NC + ic
    sqz[there] = row
    for k in sorted(range(1, NZ * NC), key=lambda k: -min(k // NC, NZ - k // NC)):
        send(sqz.at[there], sqz.at[there], qz_s.at[k - 1], qz_r.at[there], to_column(k))

    for k in (1, 3, 2):
        fx = at_x(NX - k)
        arrived(wbuf.at[ic, :, fx], wx_s.at[k - 1], wx_r.at[k - 1])
        arrived(gbuf.at[:, fx], gx_s.at[k - 1], gx_r.at[k - 1])
        send(wbuf.at[ic, :, fx], wbuf.at[ic, :, fx], wc_s.at[k], wc_r.at[k], sibling)
    for z in range(NZ):
        row = jnp.zeros((1, 128), F32)
        for xx in range(NX):
            for yl in range(NYL):
                row = row + gbuf[z, xx, yl]
        gainrow[:, z * 128 : (z + 1) * 128] = jnp.broadcast_to(row, (8, 128))
    hbuf[:, width:] = jnp.zeros((tokens, 128), F32)
    for k in range(NX):
        fx = at_x(NX - k)
        arrived(wbuf.at[oc, :, fx], wc_s.at[k], wc_r.at[k])

    @pl.loop(0, NG)
    def _(n):
        cols = pl.ds(pl.multiple_of(n * 256, 256), 256)
        dims = (((1,), (1,)), ((), ()))
        h = jnp.zeros((tokens, 256), F32)
        for half in range(2):
            wt = wbuf[half, pl.ds(n * 2, 2)].reshape(256, 256)
            h = h + lax.dot_general(
                vg_ref[:, half * 256 : half * 256 + 256], wt, dims, preferred_element_type=F32
            )
        h = h * gainrow[0:1, cols]
        hbuf[:, cols] = h
        hx = h * x_ref[:, cols].astype(F32)
        hbuf[:, width:] += hx[:, :128] + hx[:, 128:]

    @pl.loop(0, tokens // block)
    def _(t):
        rows = pl.ds(pl.multiple_of(t * block, block), block)
        inner = jnp.sum(hbuf[rows, width:], axis=1, keepdims=True) / width
        inv = rstd[rows, 0:1]
        coef = inv * inv * inv * inner
        for j in range(width // 128):
            cs = slice(j * 128, (j + 1) * 128)
            v = x_ref[rows, cs].astype(F32)
            out_ref[rows, cs] = (inv * hbuf[rows, cs] - v * coef).astype(BF16)

    for k in range(1, NYH * NC):
        fh, fc = lax.rem(ih + NYH - k // NC, NYH), lax.rem(ic + k % NC, NC)
        arrived(gb.at[fh, fc], rg_s.at[k - 1], rg_r.at[k - 1])
    for k in range(1, NZ * NC):
        there = at_z(k // NC) * NC + lax.rem(ic + k % NC, NC)
        arrived(sqz.at[there], qz_s.at[0], qz_r.at[there])
    row = sqz[0]
    for k in range(1, NZ * NC):
        row = row + sqz[k]
    squares = jnp.sum(row, axis=1, keepdims=True)
    factor = 1.0 / jnp.maximum(1.0, jnp.sqrt(squares / (width * 512)))
    for hh in range(NYH):
        for cc in range(NC):
            upd_ref[cc * 8 : cc * 8 + 8, hh * 128 : hh * 128 + 128] = gb[hh, cc] * factor

    for copy in sends:
        copy.wait_send()

    @pl.loop(0, NG)
    def _(n):
        core_copy(n).wait_send()
        for k in range(1, NX):
            x_copy(k, n).wait_send()
        for k in range(1, NY):
            y_copy(k, n).wait_send()

    @pl.loop(0, NG - 1)
    def _(n):
        for zl in range(2):
            z_copy(zl, n).wait_send()

    z_copy(1 - parity, NG - 1).wait_send()


def on_device(activations, value_grad, norm_gain, value_weight):
    batch, tok, width = activations.shape
    columns = value_grad.shape[2]
    tokens = batch * tok
    own = norm_gain.shape[0]
    gain = norm_gain.astype(F32)
    place = lax.axis_index("x") * NYL + lax.axis_index("yl")
    lanes = jnp.arange(128) // own == place
    grow = jnp.where(lanes, jnp.tile(gain, 128 // own), 0.0).reshape(1, 128)
    gcol = jnp.broadcast_to(gain.reshape(NC, own // NC, 1), (NC, own // NC, 128))
    weight = jnp.moveaxis(value_weight.reshape(own, NC, columns // NC), 1, 0)
    vm = pl.BlockSpec(memory_space=pltpu.VMEM)
    hbm = pl.BlockSpec(memory_space=pltpu.HBM)
    dma = pltpu.SemaphoreType.DMA

    def sem(*n):
        kind = dma(n) if n else dma
        return [kind, kind]

    v = pltpu.VMEM
    scratch = [
        v((tokens, width), BF16),
        v((tokens, columns), BF16),
        v((tokens, 128), F32),
        v((tokens, columns), BF16),
        v((tokens, columns), BF16),
        v((NC, NG, NX, NY, 16, 128), F32),
        v((NG, NX, NY, 16, 128), F32),
        v((NX - 1, NG, NY, 16, 128), BF16),
        v((NX - 1, NG, NY, 16, 128), BF16),
        v((NG, NY, 16, 128), F32),
        v((len(FAR), NG, 16, 128), BF16),
        v((len(NEAR), NG, 16, 128), F32),
        v((len(FAR), NG, 16, 128), BF16),
        v((NG, 16, 128), F32),
        v((NZ, 8, 128), F32),
        v((NYH, NC, 8, 128), F32),
        v((NX * NY, 1, 128), F32),
        v((NZ * NC, 1, 128), F32),
        v((NC, NZ, NX, NYL, own, columns // NC), BF16),
        v((NZ, NX, NYL, 1, 128), F32),
        v((tokens, width + 128), F32),
        v((8, width), F32),
        dma((5,)),
        *sem(NZ - 1), *sem(NZ - 1), *sem(), *sem(), *sem(NX - 1), *sem(NX - 1), *sem(NX),
        *sem(NG), *sem(NX - 1, NG), *sem(NY - 1, NG), dma((NG, 2)), dma((NZ,)),
        *sem(NYH * NC - 1), dma((NX * NY - 1,)), dma((NX * NY,)),
        dma((NZ * NC - 1,)), dma((NZ * NC,)),
    ]
    result, update = pl.pallas_call(
        kernel,
        out_shape=(
            jax.ShapeDtypeStruct((tokens, width), BF16),
            jax.ShapeDtypeStruct((own, columns), F32),
        ),
        in_specs=[hbm, hbm, vm, vm, vm],
        out_specs=(vm, vm),
        scratch_shapes=scratch,
        compiler_params=pltpu.CompilerParams(
            collective_id=0, has_side_effects=True, vmem_limit_bytes=48 * 1024 * 1024
        ),
        name="normed_value_backward",
    )(activations.reshape(tokens, width), value_grad.reshape(tokens, columns), weight, grow, gcol)
    return result.reshape(activations.shape), update


def solution(mesh):
    split = Mesh(mesh.devices.reshape(NZ, NX, NYL, NYH, NC), AXES)
    rows = ("z", "x", "yl")
    placed = (P(None, AXES, None), P(None, AXES, None), P(rows), P(rows, None))
    return jax.shard_map(
        on_device,
        mesh=split,
        in_specs=placed,
        out_specs=(P(None, AXES, None), P(rows, None)),
        check_vma=False,
    )
```

```python
import jax
import jax.numpy as jnp
from jax import lax
from jax.experimental import pallas as pl
from jax.experimental.pallas import tpu as pltpu
from jax.sharding import Mesh
from jax.sharding import PartitionSpec as P

AXES = ("z", "x", "yl", "yh", "c")
NZ, NX, NYL, NYH, NC = 16, 4, 2, 4, 2
NY = NYL * NYH
NG = NZ // 2
FAR = (4, 3, 5)
NEAR = (2, 6, 1, 7)
MESH = pl.DeviceIdType.MESH
F32, BF16 = jnp.float32, jnp.bfloat16


def kernel(
    x_hbm, vg_hbm, gain_hbm, w_hbm,
    out_ref, upd_ref,
    x_ref, vg_ref, w_ref, gain_ref, grow_ref, gcol_ref, rstd, hi, lo, g, r, xs, xr, s, sb, yr, yb, s2, zr, gb, sqp, sqz,
    wbuf, gbuf, hbuf, gainrow,
    ld, wz_s, wz_r, gz_s, gz_r, wy_s, wy_r, gy_s, gy_r, wx_s, wx_r, gx_s, gx_r, wc_s, wc_r,
    dc_s, dc_r, rx_s, rx_r, ry_s, ry_r, rz_s, rz_r, rg_s, rg_r, qp_s, qp_r, qz_s, qz_r,
):
    iz, ix, il, ih, ic = (lax.axis_index(a) for a in AXES)
    iy = ih * NYL + il
    parity = lax.rem(iz, 2)
    tokens, width = x_ref.shape
    oc = 1 - ic
    sibling = {"c": oc}
    sends = []

    def at_x(k):
        return lax.rem(ix + k, NX)

    def at_y(k):
        return lax.rem(iy + k, NY)

    def at_z(k):
        return lax.rem(iz + k, NZ)

    def to_x(k):
        return {"x": at_x(k)}

    def to_y(k):
        y = at_y(k)
        return {"yh": y // NYL, "yl": lax.rem(y, NYL)}

    def to_rep(k):
        return {"yh": lax.rem(ih + k // NC, NYH), "c": lax.rem(ic + k % NC, NC)}

    def to_plane(k):
        return {"x": at_x(k // NY), **to_y(k % NY)}

    def to_column(k):
        return {"z": at_z(k // NC), "c": lax.rem(ic + k % NC, NC)}

    def remote(src, dst, ss, rs, dev):
        return pltpu.make_async_remote_copy(
            src_ref=src, dst_ref=dst, send_sem=ss, recv_sem=rs, device_id=dev, device_id_type=MESH
        )

    def send(*args):
        copy = remote(*args)
        copy.start()
        sends.append(copy)

    def arrived(dst, ss, rs):
        remote(dst, dst, ss, rs, sibling).wait_recv()

    parts = ld.shape[0] - 4
    chunk = tokens // parts
    loads = [
        pltpu.make_async_copy(
            x_hbm.at[pl.ds(t * chunk, chunk)], x_ref.at[pl.ds(t * chunk, chunk)], ld.at[t]
        )
        for t in range(parts)
    ]
    loads.append(pltpu.make_async_copy(vg_hbm, vg_ref, ld.at[parts]))
    for h in range(NC):
        cols = pl.ds(h * w_ref.shape[2], w_ref.shape[2])
        loads.append(
            pltpu.make_async_copy(w_hbm.at[:, cols], w_ref.at[h], ld.at[parts + 1 + h])
        )
    loads.append(pltpu.make_async_copy(gain_hbm, gain_ref, ld.at[parts + 3]))
    for t in (0, parts, *range(1, parts), *range(parts + 1, parts + 4)):
        loads[t].start()

    barrier = pltpu.get_barrier_semaphore()
    peers = [to_column(k) for k in range(1, NZ * NC)]
    peers += [to_plane(k) for k in range(1, NX * NY)]
    peers += [to_rep(k) for k in range(1, NYH * NC) if k % NC and k // NC]
    for dev in peers:
        pl.semaphore_signal(barrier, inc=1, device_id=dev, device_id_type=MESH)


    block = 64
    for t in range(parts):
        loads[t].wait()
        if t == 0:
            loads[parts].wait()

        @pl.loop(t * chunk // block, (t + 1) * chunk // block)
        def _(b):
            rows = pl.ds(pl.multiple_of(b * block, block), block)
            acc = jnp.zeros((block, 128), F32)
            for j in range(width // 128):
                v = x_ref[rows, j * 128 : (j + 1) * 128].astype(F32)
                acc = acc + v * v
            inv = lax.rsqrt(jnp.sum(acc, axis=1, keepdims=True) / width + 1e-05)
            rstd[rows, :] = jnp.broadcast_to(inv, (block, 128))
            scaled = vg_ref[rows, :].astype(F32) * inv
            high = scaled.astype(BF16)
            hi[rows, :] = high
            lo[rows, :] = (scaled - high.astype(F32)).astype(BF16)

    for t in range(parts + 1, parts + 4):
        loads[t].wait()
    wbuf[ic, iz, ix, il] = w_ref[ic]
    own = gain_ref.shape[1]
    spread = jnp.broadcast_to(gain_ref[...].astype(F32), (own, own))
    r_at = lax.broadcasted_iota(jnp.int32, (own, own), 0)
    diagonal = jnp.where(
        r_at == lax.broadcasted_iota(jnp.int32, (own, own), 1), spread, 0.0
    ).astype(BF16)
    gcol = jnp.dot(diagonal, jnp.ones((own, 128), BF16), preferred_element_type=F32)
    for cc in range(NC):
        gcol_ref[cc] = gcol[cc * 8 : cc * 8 + 8]
    lane = lax.broadcasted_iota(jnp.int32, (own, 128), 1) - (ix * NYL + il) * own
    chosen = lane == lax.broadcasted_iota(jnp.int32, (own, 128), 0)
    grow_ref[...] = jnp.sum(jnp.where(chosen, gcol, 0.0), axis=0, keepdims=True)
    gbuf[iz, ix, il] = grow_ref[...]

    def group(n):
        half = (n + 1) // 2
        return lax.rem(iz // 2 + NG // 2 + half * (1 - 2 * (n % 2)), NG)

    def gradient(n):
        cols = pl.ds(pl.multiple_of(group(n) * 256, 256), 256)
        xa = x_ref[:, cols]
        for half in range(2):
            hc = slice(half * 256, half * 256 + 256)
            dims = (((0,), (0,)), ((), ()))
            o = lax.dot_general(xa, hi[:, hc], dims, preferred_element_type=F32)
            o = o + lax.dot_general(xa, lo[:, hc], dims, preferred_element_type=F32)
            for zl in range(2):
                for xx in range(NX):
                    for yl in range(NYL):
                        for cc in range(NC):
                            row = zl * 128 + xx * 32 + yl * 16 + cc * 8
                            for hh in range(2):
                                yy = (half * 2 + hh) * NYL + yl
                                g[cc, n, xx, yy, zl * 8 : zl * 8 + 8, :] = o[
                                    row : row + 8, hh * 128 : hh * 128 + 128
                                ]

    def core_copy(n):
        return remote(g.at[oc, n], r.at[n], dc_s.at[n], dc_r.at[n], sibling)

    def x_copy(k, n):
        return remote(
            xs.at[k - 1, n], xr.at[k - 1, n], rx_s.at[k - 1, n], rx_r.at[k - 1, n], to_x(k)
        )

    def y_copy(k, n):
        y = at_y(k)
        if k in FAR:
            j = FAR.index(k)
            src, dst = sb.at[j, n], yb.at[j, n]
        else:
            src, dst = s.at[n, y], yr.at[NEAR.index(k), n]
        return remote(src, dst, ry_s.at[k - 1, n], ry_r.at[k - 1, n], to_y(k))

    def z_copy(zl, n):
        rows = pl.ds(pl.multiple_of(zl * 8, 8), 8)
        return remote(
            s2.at[n, rows], zr.at[iz], rz_s.at[n, zl], rz_r.at[iz], {"z": group(n) * 2 + zl}
        )

    def reduce_x(n):
        core_copy(n).wait_recv()
        for k in (2, 1, 3):
            tx = at_x(k)
            xs[k - 1, n] = (g[ic, n, tx] + r[n, tx]).astype(BF16)
            x_copy(k, n).start()

    def reduce_y(n):
        for k in range(1, NX):
            x_copy(k, n).wait_recv()
        total = g[ic, n, ix] + r[n, ix]
        for k in range(1, NX):
            total = total + xr[k - 1, n].astype(F32)
        s[n] = total
        for j, k in enumerate(FAR):
            sb[j, n] = s[n, at_y(k)].astype(BF16)
        for k in FAR + NEAR:
            y_copy(k, n).start()

    def reduce_z(n):
        total = s[n, iy]
        for k in FAR + NEAR:
            y_copy(k, n).wait_recv()
            total = total + (
                yb[FAR.index(k), n].astype(F32) if k in FAR else yr[NEAR.index(k), n]
            )
        s2[n] = total

    gradient(0)
    gradient(1)
    pl.semaphore_wait(barrier, len(peers))
    core_copy(0).start()
    core_copy(1).start()

    for k in sorted(range(1, NZ), key=lambda k: -min(k, NZ - k)):
        dev = {"z": at_z(k)}
        send(w_ref.at[ic], wbuf.at[ic, iz, ix, il], wz_s.at[k - 1], wz_r.at[k - 1], dev)
        send(grow_ref, gbuf.at[iz, ix, il], gz_s.at[k - 1], gz_r.at[k - 1], dev)

    lag = 3

    @pl.loop(2, NG)
    def _(n):
        gradient(n)
        core_copy(n).start()

        @pl.when(n >= lag)
        def _():
            reduce_x(n - lag)

    @pl.loop(NG - lag, NG)
    def _(n):
        reduce_x(n)

    @pl.loop(0, 3)
    def _(n):
        reduce_y(n)

    behind = 3

    def reduce_yz(n):
        reduce_y(n)
        reduce_z(n - behind)
        for zl in range(2):
            z_copy(zl, n - behind).start()

    @pl.loop(3, 6)
    def _(n):
        reduce_yz(n)

    for k in range(1, NZ):
        fz = at_z(NZ - k)
        arrived(wbuf.at[ic, fz, ix, il], wz_s.at[k - 1], wz_r.at[k - 1])
        arrived(gbuf.at[fz, ix, il], gz_s.at[k - 1], gz_r.at[k - 1])
    send(wbuf.at[ic, :, ix, il], wbuf.at[ic, :, ix, il], wy_s, wy_r, {"yl": 1 - il})
    send(gbuf.at[:, ix, il], gbuf.at[:, ix, il], gy_s, gy_r, {"yl": 1 - il})

    @pl.loop(6, NG)
    def _(n):
        reduce_yz(n)

    arrived(wbuf.at[ic, :, ix, 1 - il], wy_s, wy_r)
    arrived(gbuf.at[:, ix, 1 - il], gy_s, gy_r)
    for k in (2, 1, 3):
        send(wbuf.at[ic, :, ix], wbuf.at[ic, :, ix], wx_s.at[k - 1], wx_r.at[k - 1], to_x(k))
        send(gbuf.at[:, ix], gbuf.at[:, ix], gx_s.at[k - 1], gx_r.at[k - 1], to_x(k))
    send(wbuf.at[ic, :, ix], wbuf.at[ic, :, ix], wc_s.at[0], wc_r.at[0], sibling)

    @pl.loop(NG - behind, NG - 1)
    def _(n):
        reduce_z(n)
        for zl in range(2):
            z_copy(zl, n).start()

    reduce_z(NG - 1)
    z_copy(1 - parity, NG - 1).start()

    own = s2[NG - 1, pl.ds(pl.multiple_of(parity * 8, 8), 8), :]
    for k in sorted(range(1, NZ), key=lambda k: -min(k, NZ - k)):
        fz = at_z(k)
        arrived(zr.at[fz], rz_s.at[0, 0], rz_r.at[fz])
        own = own + zr[fz]
    piece = own * gcol_ref[ic]
    gb[ih, ic] = piece
    there = iz * NC + ic
    sqz[there] = jnp.sum(piece * piece, axis=0, keepdims=True)
    for k in sorted(range(1, NZ * NC), key=lambda k: -min(k // NC, NZ - k // NC)):
        send(sqz.at[there], sqz.at[there], qz_s.at[k - 1], qz_r.at[there], to_column(k))
    for k in range(1, NYH * NC):
        send(gb.at[ih, ic], gb.at[ih, ic], rg_s.at[k - 1], rg_r.at[k - 1], to_rep(k))
    for k in range(1, NZ * NC):
        there = at_z(k // NC) * NC + lax.rem(ic + k % NC, NC)
        arrived(sqz.at[there], qz_s.at[0], qz_r.at[there])
    row = sqz[0]
    for k in range(1, NZ * NC):
        row = row + sqz[k]

    here = ix * NY + iy
    sqp[here] = row
    for k in sorted(range(1, NX * NY), key=lambda k: -min(k % NY, NY - k % NY)):
        send(sqp.at[here], sqp.at[here], qp_s.at[k - 1], qp_r.at[here], to_plane(k))

    for k in (1, 3, 2):
        fx = at_x(NX - k)
        arrived(wbuf.at[ic, :, fx], wx_s.at[k - 1], wx_r.at[k - 1])
        arrived(gbuf.at[:, fx], gx_s.at[k - 1], gx_r.at[k - 1])
        send(wbuf.at[ic, :, fx], wbuf.at[ic, :, fx], wc_s.at[k], wc_r.at[k], sibling)
    for z in range(NZ):
        row = jnp.zeros((1, 128), F32)
        for xx in range(NX):
            for yl in range(NYL):
                row = row + gbuf[z, xx, yl]
        gainrow[:, z * 128 : (z + 1) * 128] = jnp.broadcast_to(row, (8, 128))
    hbuf[:, width:] = jnp.zeros((tokens, 128), F32)
    for k in range(NX):
        fx = at_x(NX - k)
        arrived(wbuf.at[oc, :, fx], wc_s.at[k], wc_r.at[k])

    @pl.loop(0, NG)
    def _(n):
        cols = pl.ds(pl.multiple_of(n * 256, 256), 256)
        dims = (((1,), (1,)), ((), ()))
        h = jnp.zeros((tokens, 256), F32)
        for half in range(2):
            wt = wbuf[half, pl.ds(n * 2, 2)].reshape(256, 256)
            h = h + lax.dot_general(
                vg_ref[:, half * 256 : half * 256 + 256], wt, dims, preferred_element_type=F32
            )
        h = h * gainrow[0:1, cols]
        hbuf[:, cols] = h
        hx = h * x_ref[:, cols].astype(F32)
        hbuf[:, width:] += hx[:, :128] + hx[:, 128:]

    @pl.loop(0, tokens // block)
    def _(t):
        rows = pl.ds(pl.multiple_of(t * block, block), block)
        inner = jnp.sum(hbuf[rows, width:], axis=1, keepdims=True) / width
        inv = rstd[rows, 0:1]
        coef = inv * inv * inv * inner
        for j in range(width // 128):
            cs = slice(j * 128, (j + 1) * 128)
            v = x_ref[rows, cs].astype(F32)
            out_ref[rows, cs] = (inv * hbuf[rows, cs] - v * coef).astype(BF16)

    for k in range(1, NYH * NC):
        fh, fc = lax.rem(ih + NYH - k // NC, NYH), lax.rem(ic + k % NC, NC)
        arrived(gb.at[fh, fc], rg_s.at[k - 1], rg_r.at[k - 1])
    for k in range(1, NX * NY):
        there = at_x(k // NY) * NY + at_y(k % NY)
        arrived(sqp.at[there], qp_s.at[0], qp_r.at[there])
    row = sqp[0]
    for k in range(1, NX * NY):
        row = row + sqp[k]
    squares = jnp.sum(row, axis=1, keepdims=True)
    factor = 1.0 / jnp.maximum(1.0, jnp.sqrt(squares / (width * 512)))
    for hh in range(NYH):
        for cc in range(NC):
            upd_ref[cc * 8 : cc * 8 + 8, hh * 128 : hh * 128 + 128] = gb[hh, cc] * factor

    for copy in sends:
        copy.wait_send()

    @pl.loop(0, NG)
    def _(n):
        core_copy(n).wait_send()
        for k in range(1, NX):
            x_copy(k, n).wait_send()
        for k in range(1, NY):
            y_copy(k, n).wait_send()

    @pl.loop(0, NG - 1)
    def _(n):
        for zl in range(2):
            z_copy(zl, n).wait_send()

    z_copy(1 - parity, NG - 1).wait_send()


def on_device(activations, value_grad, norm_gain, value_weight):
    batch, tok, width = activations.shape
    columns = value_grad.shape[2]
    tokens = batch * tok
    own = norm_gain.shape[0]
    vm = pl.BlockSpec(memory_space=pltpu.VMEM)
    hbm = pl.BlockSpec(memory_space=pltpu.HBM)
    dma = pltpu.SemaphoreType.DMA

    def sem(*n):
        kind = dma(n) if n else dma
        return [kind, kind]

    v = pltpu.VMEM
    scratch = [
        v((tokens, width), BF16),
        v((tokens, columns), BF16),
        v((NC, own, columns // NC), BF16),
        v((1, own), BF16),
        v((1, 128), F32),
        v((NC, own // NC, 128), F32),
        v((tokens, 128), F32),
        v((tokens, columns), BF16),
        v((tokens, columns), BF16),
        v((NC, NG, NX, NY, 16, 128), F32),
        v((NG, NX, NY, 16, 128), F32),
        v((NX - 1, NG, NY, 16, 128), BF16),
        v((NX - 1, NG, NY, 16, 128), BF16),
        v((NG, NY, 16, 128), F32),
        v((len(FAR), NG, 16, 128), BF16),
        v((len(NEAR), NG, 16, 128), F32),
        v((len(FAR), NG, 16, 128), BF16),
        v((NG, 16, 128), F32),
        v((NZ, 8, 128), F32),
        v((NYH, NC, 8, 128), F32),
        v((NX * NY, 1, 128), F32),
        v((NZ * NC, 1, 128), F32),
        v((NC, NZ, NX, NYL, own, columns // NC), BF16),
        v((NZ, NX, NYL, 1, 128), F32),
        v((tokens, width + 128), F32),
        v((8, width), F32),
        dma((8,)),
        *sem(NZ - 1), *sem(NZ - 1), *sem(), *sem(), *sem(NX - 1), *sem(NX - 1), *sem(NX),
        *sem(NG), *sem(NX - 1, NG), *sem(NY - 1, NG), dma((NG, 2)), dma((NZ,)),
        *sem(NYH * NC - 1), dma((NX * NY - 1,)), dma((NX * NY,)),
        dma((NZ * NC - 1,)), dma((NZ * NC,)),
    ]
    operands = (
        activations.reshape(tokens, width),
        value_grad.reshape(tokens, columns),
        norm_gain.reshape(1, own),
        value_weight,
    )
    result, update = pl.pallas_call(
        kernel,
        out_shape=(
            jax.ShapeDtypeStruct((tokens, width), BF16),
            jax.ShapeDtypeStruct((own, columns), F32),
        ),
        in_specs=[hbm] * 4,
        out_specs=(vm, vm),
        scratch_shapes=scratch,
        compiler_params=pltpu.CompilerParams(
            collective_id=0, has_side_effects=True, vmem_limit_bytes=48 * 1024 * 1024
        ),
        name="normed_value_backward",
    )(*(pltpu.with_memory_space_constraint(a, pltpu.HBM) for a in operands))
    return result.reshape(activations.shape), update


def solution(mesh):
    split = Mesh(mesh.devices.reshape(NZ, NX, NYL, NYH, NC), AXES)
    rows = ("z", "x", "yl")
    placed = (P(None, AXES, None), P(None, AXES, None), P(rows), P(rows, None))
    return jax.shard_map(
        on_device,
        mesh=split,
        in_specs=placed,
        out_specs=(P(None, AXES, None), P(rows, None)),
        check_vma=False,
    )
```

```python
import jax
import jax.numpy as jnp
from jax import lax
from jax.experimental import pallas as pl
from jax.experimental.pallas import tpu as pltpu
from jax.sharding import Mesh
from jax.sharding import PartitionSpec as P

AXES = ("z", "x", "yl", "yh", "c")
NZ, NX, NYL, NYH, NC = 16, 4, 2, 4, 2
NY = NYL * NYH
NG = NZ // 2
FAR = (4, 3, 5)
NEAR = (2, 6, 1, 7)
MESH = pl.DeviceIdType.MESH
F32, BF16 = jnp.float32, jnp.bfloat16


def kernel(
    x_hbm, vg_hbm, gain_hbm, w_hbm,
    out_ref, upd_ref,
    x_ref, vg_ref, w_ref, gain_ref, grow_ref, gcol_ref, rstd, hi, lo, g, r, xs, xr, s, sb, yr, yb, s2, zr, gb, sqp, sqz,
    wbuf, gbuf, hbuf, gainrow,
    ld, wz_s, wz_r, gz_s, gz_r, wy_s, wy_r, gy_s, gy_r, wx_s, wx_r, gx_s, gx_r, vx_s, vx_r, vy_s, vy_r, wc_s, wc_r,
    dc_s, dc_r, rx_s, rx_r, ry_s, ry_r, rz_s, rz_r, rg_s, rg_r, qp_s, qp_r, qz_s, qz_r,
):
    iz, ix, il, ih, ic = (lax.axis_index(a) for a in AXES)
    iy = ih * NYL + il
    parity = lax.rem(iz, 2)
    tokens, width = x_ref.shape
    oc = 1 - ic
    sibling = {"c": oc}
    sends = []

    def at_x(k):
        return lax.rem(ix + k, NX)

    def at_y(k):
        return lax.rem(iy + k, NY)

    def at_z(k):
        return lax.rem(iz + k, NZ)

    def to_x(k):
        return {"x": at_x(k)}

    def to_y(k):
        y = at_y(k)
        return {"yh": y // NYL, "yl": lax.rem(y, NYL)}

    def to_rep(k):
        return {"yh": lax.rem(ih + k // NC, NYH), "c": lax.rem(ic + k % NC, NC)}

    def to_plane(k):
        return {"x": at_x(k // NY), **to_y(k % NY)}

    def to_column(k):
        return {"z": at_z(k // NC), "c": lax.rem(ic + k % NC, NC)}

    def remote(src, dst, ss, rs, dev):
        return pltpu.make_async_remote_copy(
            src_ref=src, dst_ref=dst, send_sem=ss, recv_sem=rs, device_id=dev, device_id_type=MESH
        )

    def send(*args):
        copy = remote(*args)
        copy.start()
        sends.append(copy)

    def arrived(dst, ss, rs):
        remote(dst, dst, ss, rs, sibling).wait_recv()

    parts = ld.shape[0] - 4
    chunk = tokens // parts
    loads = [
        pltpu.make_async_copy(
            x_hbm.at[pl.ds(t * chunk, chunk)], x_ref.at[pl.ds(t * chunk, chunk)], ld.at[t]
        )
        for t in range(parts)
    ]
    loads.append(pltpu.make_async_copy(vg_hbm, vg_ref, ld.at[parts]))
    for h in range(NC):
        cols = pl.ds(h * w_ref.shape[2], w_ref.shape[2])
        loads.append(
            pltpu.make_async_copy(w_hbm.at[:, cols], w_ref.at[h], ld.at[parts + 1 + h])
        )
    loads.append(pltpu.make_async_copy(gain_hbm, gain_ref, ld.at[parts + 3]))
    for t in (0, parts, *range(1, parts), *range(parts + 1, parts + 4)):
        loads[t].start()

    barrier = pltpu.get_barrier_semaphore()
    peers = [to_column(k) for k in range(1, NZ * NC)]
    peers += [to_plane(k) for k in range(1, NX * NY)]
    peers += [to_rep(k) for k in range(1, NYH * NC) if k % NC and k // NC]
    for dev in peers:
        pl.semaphore_signal(barrier, inc=1, device_id=dev, device_id_type=MESH)


    block = 64
    for t in range(parts):
        loads[t].wait()
        if t == 0:
            loads[parts].wait()

        @pl.loop(t * chunk // block, (t + 1) * chunk // block)
        def _(b):
            rows = pl.ds(pl.multiple_of(b * block, block), block)
            acc = jnp.zeros((block, 128), F32)
            for j in range(width // 128):
                v = x_ref[rows, j * 128 : (j + 1) * 128].astype(F32)
                acc = acc + v * v
            inv = lax.rsqrt(jnp.sum(acc, axis=1, keepdims=True) / width + 1e-05)
            rstd[rows, :] = jnp.broadcast_to(inv, (block, 128))
            scaled = vg_ref[rows, :].astype(F32) * inv
            high = scaled.astype(BF16)
            hi[rows, :] = high
            lo[rows, :] = (scaled - high.astype(F32)).astype(BF16)

    for t in range(parts + 1, parts + 4):
        loads[t].wait()
    wbuf[ic, iz, ix, il] = w_ref[ic]
    own = gain_ref.shape[1]
    spread = jnp.broadcast_to(gain_ref[...].astype(F32), (own, own))
    r_at = lax.broadcasted_iota(jnp.int32, (own, own), 0)
    diagonal = jnp.where(
        r_at == lax.broadcasted_iota(jnp.int32, (own, own), 1), spread, 0.0
    ).astype(BF16)
    gcol = jnp.dot(diagonal, jnp.ones((own, 128), BF16), preferred_element_type=F32)
    for cc in range(NC):
        gcol_ref[cc] = gcol[cc * 8 : cc * 8 + 8]
    lane = lax.broadcasted_iota(jnp.int32, (own, 128), 1) - (ix * NYL + il) * own
    chosen = lane == lax.broadcasted_iota(jnp.int32, (own, 128), 0)
    grow_ref[...] = jnp.sum(jnp.where(chosen, gcol, 0.0), axis=0, keepdims=True)
    gbuf[iz, ix, il] = grow_ref[...]

    def group(n):
        half = (n + 1) // 2
        return lax.rem(iz // 2 + NG // 2 + half * (1 - 2 * (n % 2)), NG)

    def gradient(n):
        cols = pl.ds(pl.multiple_of(group(n) * 256, 256), 256)
        xa = x_ref[:, cols]
        for half in range(2):
            hc = slice(half * 256, half * 256 + 256)
            dims = (((0,), (0,)), ((), ()))
            o = lax.dot_general(xa, hi[:, hc], dims, preferred_element_type=F32)
            o = o + lax.dot_general(xa, lo[:, hc], dims, preferred_element_type=F32)
            for zl in range(2):
                for xx in range(NX):
                    for yl in range(NYL):
                        for cc in range(NC):
                            row = zl * 128 + xx * 32 + yl * 16 + cc * 8
                            for hh in range(2):
                                yy = (half * 2 + hh) * NYL + yl
                                g[cc, n, xx, yy, zl * 8 : zl * 8 + 8, :] = o[
                                    row : row + 8, hh * 128 : hh * 128 + 128
                                ]

    def core_copy(n):
        return remote(g.at[oc, n], r.at[n], dc_s.at[n], dc_r.at[n], sibling)

    def x_copy(k, n):
        return remote(
            xs.at[k - 1, n], xr.at[k - 1, n], rx_s.at[k - 1, n], rx_r.at[k - 1, n], to_x(k)
        )

    def y_copy(k, n):
        y = at_y(k)
        if k in FAR:
            j = FAR.index(k)
            src, dst = sb.at[j, n], yb.at[j, n]
        else:
            src, dst = s.at[n, y], yr.at[NEAR.index(k), n]
        return remote(src, dst, ry_s.at[k - 1, n], ry_r.at[k - 1, n], to_y(k))

    def z_copy(zl, n):
        rows = pl.ds(pl.multiple_of(zl * 8, 8), 8)
        return remote(
            s2.at[n, rows], zr.at[iz], rz_s.at[n, zl], rz_r.at[iz], {"z": group(n) * 2 + zl}
        )

    def reduce_x(n):
        core_copy(n).wait_recv()
        for k in (2, 1, 3):
            tx = at_x(k)
            xs[k - 1, n] = (g[ic, n, tx] + r[n, tx]).astype(BF16)
            x_copy(k, n).start()

    def reduce_y(n):
        for k in range(1, NX):
            x_copy(k, n).wait_recv()
        total = g[ic, n, ix] + r[n, ix]
        for k in range(1, NX):
            total = total + xr[k - 1, n].astype(F32)
        s[n] = total
        for j, k in enumerate(FAR):
            sb[j, n] = s[n, at_y(k)].astype(BF16)
        for k in FAR + NEAR:
            y_copy(k, n).start()

    def reduce_z(n):
        total = s[n, iy]
        for k in FAR + NEAR:
            y_copy(k, n).wait_recv()
            total = total + (
                yb[FAR.index(k), n].astype(F32) if k in FAR else yr[NEAR.index(k), n]
            )
        s2[n] = total

    gradient(0)
    gradient(1)
    pl.semaphore_wait(barrier, len(peers))
    core_copy(0).start()
    core_copy(1).start()

    for k in sorted(range(1, NZ), key=lambda k: -min(k, NZ - k)):
        dev = {"z": at_z(k)}
        send(w_ref.at[ic], wbuf.at[ic, iz, ix, il], wz_s.at[k - 1], wz_r.at[k - 1], dev)
        send(grow_ref, gbuf.at[iz, ix, il], gz_s.at[k - 1], gz_r.at[k - 1], dev)

    lag = 3

    @pl.loop(2, NG)
    def _(n):
        gradient(n)
        core_copy(n).start()

        @pl.when(n >= lag)
        def _():
            reduce_x(n - lag)

    @pl.loop(NG - lag, NG)
    def _(n):
        reduce_x(n)

    @pl.loop(0, 3)
    def _(n):
        reduce_y(n)

    behind = 3

    def reduce_yz(n):
        reduce_y(n)
        reduce_z(n - behind)
        for zl in range(2):
            z_copy(zl, n - behind).start()

    @pl.loop(3, 6)
    def _(n):
        reduce_yz(n)

    for k in range(1, NZ):
        fz = at_z(NZ - k)
        arrived(wbuf.at[ic, fz, ix, il], wz_s.at[k - 1], wz_r.at[k - 1])
        arrived(gbuf.at[fz, ix, il], gz_s.at[k - 1], gz_r.at[k - 1])
    left, right = pl.ds(0, 128), pl.ds(128, 128)
    mine = wbuf.at[ic, :, ix, il, :, left]
    send(mine, mine, wy_s, wy_r, {"yl": 1 - il})
    mine = wbuf.at[ic, :, ix, il, :, right]
    for k in (2, 1, 3):
        send(mine, mine, wx_s.at[k - 1], wx_r.at[k - 1], to_x(k))
    send(gbuf.at[:, ix, il], gbuf.at[:, ix, il], gy_s, gy_r, {"yl": 1 - il})

    @pl.loop(6, NG)
    def _(n):
        reduce_yz(n)

    @pl.loop(NG - behind, NG - 1)
    def _(n):
        reduce_z(n)
        for zl in range(2):
            z_copy(zl, n).start()

    reduce_z(NG - 1)
    z_copy(1 - parity, NG - 1).start()

    arrived(wbuf.at[ic, :, ix, 1 - il, :, left], wy_s, wy_r)
    arrived(gbuf.at[:, ix, 1 - il], gy_s, gy_r)
    mine = wbuf.at[ic, :, ix, :, :, left]
    for k in (2, 1, 3):
        send(mine, mine, vx_s.at[k - 1], vx_r.at[k - 1], to_x(k))
        send(gbuf.at[:, ix], gbuf.at[:, ix], gx_s.at[k - 1], gx_r.at[k - 1], to_x(k))
    for k in (1, 3, 2):
        arrived(wbuf.at[ic, :, at_x(NX - k), il, :, right], wx_s.at[k - 1], wx_r.at[k - 1])
    mine = wbuf.at[ic, :, :, il, :, right]
    send(mine, mine, vy_s, vy_r, {"yl": 1 - il})

    own = s2[NG - 1, pl.ds(pl.multiple_of(parity * 8, 8), 8), :]
    for k in sorted(range(1, NZ), key=lambda k: -min(k, NZ - k)):
        fz = at_z(k)
        arrived(zr.at[fz], rz_s.at[0, 0], rz_r.at[fz])
        own = own + zr[fz]
    piece = own * gcol_ref[ic]
    gb[ih, ic] = piece
    there = iz * NC + ic
    sqz[there] = jnp.sum(piece * piece, axis=0, keepdims=True)
    for k in sorted(range(1, NZ * NC), key=lambda k: -min(k // NC, NZ - k // NC)):
        send(sqz.at[there], sqz.at[there], qz_s.at[k - 1], qz_r.at[there], to_column(k))
    for k in range(1, NYH * NC):
        send(gb.at[ih, ic], gb.at[ih, ic], rg_s.at[k - 1], rg_r.at[k - 1], to_rep(k))
    for k in range(1, NZ * NC):
        there = at_z(k // NC) * NC + lax.rem(ic + k % NC, NC)
        arrived(sqz.at[there], qz_s.at[0], qz_r.at[there])
    row = sqz[0]
    for k in range(1, NZ * NC):
        row = row + sqz[k]

    here = ix * NY + iy
    sqp[here] = row
    for k in sorted(range(1, NX * NY), key=lambda k: -min(k % NY, NY - k % NY)):
        send(sqp.at[here], sqp.at[here], qp_s.at[k - 1], qp_r.at[here], to_plane(k))

    for k in (1, 3, 2):
        fx = at_x(NX - k)
        arrived(wbuf.at[ic, :, fx, :, :, left], vx_s.at[k - 1], vx_r.at[k - 1])
        arrived(gbuf.at[:, fx], gx_s.at[k - 1], gx_r.at[k - 1])
    arrived(wbuf.at[ic, :, :, 1 - il, :, right], vy_s, vy_r)
    send(wbuf.at[ic], wbuf.at[ic], wc_s, wc_r, sibling)
    for z in range(NZ):
        row = jnp.zeros((1, 128), F32)
        for xx in range(NX):
            for yl in range(NYL):
                row = row + gbuf[z, xx, yl]
        gainrow[:, z * 128 : (z + 1) * 128] = jnp.broadcast_to(row, (8, 128))
    hbuf[:, width:] = jnp.zeros((tokens, 128), F32)
    arrived(wbuf.at[oc], wc_s, wc_r)

    @pl.loop(0, NG)
    def _(n):
        cols = pl.ds(pl.multiple_of(n * 256, 256), 256)
        dims = (((1,), (1,)), ((), ()))
        h = jnp.zeros((tokens, 256), F32)
        for half in range(2):
            wt = wbuf[half, pl.ds(n * 2, 2)].reshape(256, 256)
            h = h + lax.dot_general(
                vg_ref[:, half * 256 : half * 256 + 256], wt, dims, preferred_element_type=F32
            )
        h = h * gainrow[0:1, cols]
        hbuf[:, cols] = h
        hx = h * x_ref[:, cols].astype(F32)
        hbuf[:, width:] += hx[:, :128] + hx[:, 128:]

    @pl.loop(0, tokens // block)
    def _(t):
        rows = pl.ds(pl.multiple_of(t * block, block), block)
        inner = jnp.sum(hbuf[rows, width:], axis=1, keepdims=True) / width
        inv = rstd[rows, 0:1]
        coef = inv * inv * inv * inner
        for j in range(width // 128):
            cs = slice(j * 128, (j + 1) * 128)
            v = x_ref[rows, cs].astype(F32)
            out_ref[rows, cs] = (inv * hbuf[rows, cs] - v * coef).astype(BF16)

    for k in range(1, NYH * NC):
        fh, fc = lax.rem(ih + NYH - k // NC, NYH), lax.rem(ic + k % NC, NC)
        arrived(gb.at[fh, fc], rg_s.at[k - 1], rg_r.at[k - 1])
    for k in range(1, NX * NY):
        there = at_x(k // NY) * NY + at_y(k % NY)
        arrived(sqp.at[there], qp_s.at[0], qp_r.at[there])
    row = sqp[0]
    for k in range(1, NX * NY):
        row = row + sqp[k]
    squares = jnp.sum(row, axis=1, keepdims=True)
    factor = 1.0 / jnp.maximum(1.0, jnp.sqrt(squares / (width * 512)))
    for hh in range(NYH):
        for cc in range(NC):
            upd_ref[cc * 8 : cc * 8 + 8, hh * 128 : hh * 128 + 128] = gb[hh, cc] * factor

    for copy in sends:
        copy.wait_send()

    @pl.loop(0, NG)
    def _(n):
        core_copy(n).wait_send()
        for k in range(1, NX):
            x_copy(k, n).wait_send()
        for k in range(1, NY):
            y_copy(k, n).wait_send()

    @pl.loop(0, NG - 1)
    def _(n):
        for zl in range(2):
            z_copy(zl, n).wait_send()

    z_copy(1 - parity, NG - 1).wait_send()


def on_device(activations, value_grad, norm_gain, value_weight):
    batch, tok, width = activations.shape
    columns = value_grad.shape[2]
    tokens = batch * tok
    own = norm_gain.shape[0]
    vm = pl.BlockSpec(memory_space=pltpu.VMEM)
    hbm = pl.BlockSpec(memory_space=pltpu.HBM)
    dma = pltpu.SemaphoreType.DMA

    def sem(*n):
        kind = dma(n) if n else dma
        return [kind, kind]

    v = pltpu.VMEM
    scratch = [
        v((tokens, width), BF16),
        v((tokens, columns), BF16),
        v((NC, own, columns // NC), BF16),
        v((1, own), BF16),
        v((1, 128), F32),
        v((NC, own // NC, 128), F32),
        v((tokens, 128), F32),
        v((tokens, columns), BF16),
        v((tokens, columns), BF16),
        v((NC, NG, NX, NY, 16, 128), F32),
        v((NG, NX, NY, 16, 128), F32),
        v((NX - 1, NG, NY, 16, 128), BF16),
        v((NX - 1, NG, NY, 16, 128), BF16),
        v((NG, NY, 16, 128), F32),
        v((len(FAR), NG, 16, 128), BF16),
        v((len(NEAR), NG, 16, 128), F32),
        v((len(FAR), NG, 16, 128), BF16),
        v((NG, 16, 128), F32),
        v((NZ, 8, 128), F32),
        v((NYH, NC, 8, 128), F32),
        v((NX * NY, 1, 128), F32),
        v((NZ * NC, 1, 128), F32),
        v((NC, NZ, NX, NYL, own, columns // NC), BF16),
        v((NZ, NX, NYL, 1, 128), F32),
        v((tokens, width + 128), F32),
        v((8, width), F32),
        dma((8,)),
        *sem(NZ - 1), *sem(NZ - 1), *sem(), *sem(), *sem(NX - 1), *sem(NX - 1),
        *sem(NX - 1), *sem(), *sem(),
        *sem(NG), *sem(NX - 1, NG), *sem(NY - 1, NG), dma((NG, 2)), dma((NZ,)),
        *sem(NYH * NC - 1), dma((NX * NY - 1,)), dma((NX * NY,)),
        dma((NZ * NC - 1,)), dma((NZ * NC,)),
    ]
    operands = (
        activations.reshape(tokens, width),
        value_grad.reshape(tokens, columns),
        norm_gain.reshape(1, own),
        value_weight,
    )
    result, update = pl.pallas_call(
        kernel,
        out_shape=(
            jax.ShapeDtypeStruct((tokens, width), BF16),
            jax.ShapeDtypeStruct((own, columns), F32),
        ),
        in_specs=[hbm] * 4,
        out_specs=(vm, vm),
        scratch_shapes=scratch,
        compiler_params=pltpu.CompilerParams(
            collective_id=0, has_side_effects=True, vmem_limit_bytes=48 * 1024 * 1024
        ),
        name="normed_value_backward",
    )(*(pltpu.with_memory_space_constraint(a, pltpu.HBM) for a in operands))
    return result.reshape(activations.shape), update


def solution(mesh):
    split = Mesh(mesh.devices.reshape(NZ, NX, NYL, NYH, NC), AXES)
    rows = ("z", "x", "yl")
    placed = (P(None, AXES, None), P(None, AXES, None), P(rows), P(rows, None))
    return jax.shard_map(
        on_device,
        mesh=split,
        in_specs=placed,
        out_specs=(P(None, AXES, None), P(rows, None)),
        check_vma=False,
    )
```
